256 devices in a mesh: lat: 32 (over z, y_lo, core), lon: 8 (over x, y_hi).
Axes of the slice: x: 4, y: 4 (y_hi: 2, y_lo: 2; y = y_hi * 2 + y_lo), z: 8, core: 2. Of those that a mesh axis runs over, the one named last changes fastest.
Arguments:
- eastward_speed_face: float32 [72, 1024, 1024], P(None, 'lat', 'lon'), may hold values from -6 to 6
- northward_speed_face: float32 [72, 1024, 1024], P(None, 'lat', 'lon'), may hold values from -6 to 6
- stratum_extent_east_face: float32 [72, 1024, 1024], P(None, 'lat', 'lon'), may hold values from 0.5 to 2
- stratum_extent_north_face: float32 [72, 1024, 1024], P(None, 'lat', 'lon'), may hold values from 0.5 to 2
- northward_span_east_face: float32 [1024, 1024], P('lat', 'lon'), may hold values from 0.5 to 2
- eastward_span_north_face: float32 [1024, 1024], P('lat', 'lon'), may hold values from 0.5 to 2
- ocean_flag_east_face: int32 [72, 1024, 1024], P(None, 'lat', 'lon'), may hold values 0 or 1
- ocean_flag_north_face: int32 [72, 1024, 1024], P(None, 'lat', 'lon'), may hold values 0 or 1
- counterpart_across_seam: int32 [1024], replicated, may hold values from 0 to 1023, as said below
Outputs:
- eastward_speed_next: float32 [72, 1024, 1024], P(None, 'lat', 'lon')
- northward_speed_next: float32 [72, 1024, 1024], P(None, 'lat', 'lon')
The draws below stay inside these ranges and needn't reach their ends.
Inputs may be any that keep to these rules, and one draw needn't show every extreme that they name: counterpart_across_seam[i] = (p - 1 - i) mod 1024 for one pivot p drawn anew in each draw; it is its own inverse.
All inputs are finite; a program needn't handle non-finite values. No bound on the sum of `ocean_flag_east_face` or of `ocean_flag_north_face` on one device may be relied on, other than what follows from the above.
Results may differ from the reference program's by a relative error of at most 0.00002.
Values sent between devices are 32-bit elements; how exact they have to be, the bound alone decides.
A program may use at most 128 MiB of HBM per device.

```python
import math
import jax
import jax.numpy as jnp
from jax import lax

STRATA_COUNT = 72
NORTHWARD_CELLS = 1024
EASTWARD_CELLS = 1024


def draw_counterpart_across_seam(key, part):
    pivot = jax.random.randint(jax.random.fold_in(key, 17), (), 0, EASTWARD_CELLS)
    columns = jnp.arange(EASTWARD_CELLS, dtype=jnp.int32)
    return ((pivot - 1 - columns) % EASTWARD_CELLS).astype(jnp.int32)


def touch_ends(values, rng, low, high):
    longest = values.shape.index(max(values.shape))
    spots = []
    for shift in (0, 1):
        where = [jax.random.randint(jax.random.fold_in(rng, axis), (), 0, length) for axis, length in enumerate(values.shape)]
        where[longest] = (where[longest] + shift) % values.shape[longest]
        spots.append(tuple(where))
    return values.at[spots[0]].set(low).at[spots[1]].set(high)


def shard_levels(rng, shape, pieces, least, top_value):
    def one(dim, parts):
        draws = jax.random.uniform(jax.random.fold_in(jax.random.fold_in(rng, 6), dim), (parts,), jnp.float32, least / len(pieces), top_value / len(pieces))
        return jnp.repeat(jnp.exp(draws), shape[dim] // parts).reshape((-1,) + (1,) * (len(shape) - dim - 1))

    loudness = one(*pieces[0])
    for cut in pieces[1:]:
        loudness = loudness * one(*cut)
    return loudness


def centred(key, shape, scale, most, pieces=(), kind=jnp.bfloat16):
    loudness = shard_levels(key, shape, pieces, -0.22, 0.18) if pieces else 1.0
    values = jax.random.normal(key, shape, jnp.float32) * scale * loudness
    return jnp.minimum(jnp.maximum(values, -most), most).astype(kind)


def setup_inputs(seed: int = 0) -> dict:
    key_of = jax.random.split(jax.random.key(seed), 10)
    return {
        "eastward_speed_face": centred(key_of[0], (STRATA_COUNT, NORTHWARD_CELLS, EASTWARD_CELLS), 1.0, 6.0, ((1, 32), (2, 8)), jnp.float32),
        "northward_speed_face": centred(key_of[1], (STRATA_COUNT, NORTHWARD_CELLS, EASTWARD_CELLS), 1.0, 6.0, ((1, 32), (2, 8)), jnp.float32),
        "stratum_extent_east_face": jnp.clip(jnp.exp(math.log(2.0) - 1.3862944 * jax.random.uniform(key_of[2], (STRATA_COUNT, NORTHWARD_CELLS, EASTWARD_CELLS), jnp.float32) ** shard_levels(key_of[2], (STRATA_COUNT, NORTHWARD_CELLS, EASTWARD_CELLS), ((1, 32), (2, 8)), -0.2, 0.2)), 0.5, 2.0),
        "stratum_extent_north_face": jnp.clip(jnp.exp(math.log(2.0) - 1.3862944 * jax.random.uniform(key_of[3], (STRATA_COUNT, NORTHWARD_CELLS, EASTWARD_CELLS), jnp.float32) ** shard_levels(key_of[3], (STRATA_COUNT, NORTHWARD_CELLS, EASTWARD_CELLS), ((1, 32), (2, 8)), -0.2, 0.2)), 0.5, 2.0),
        "northward_span_east_face": jnp.clip(jnp.exp(math.log(2.0) - 1.3862944 * jax.random.uniform(key_of[4], (NORTHWARD_CELLS, EASTWARD_CELLS), jnp.float32) ** shard_levels(key_of[4], (NORTHWARD_CELLS, EASTWARD_CELLS), ((0, 32), (1, 8)), -0.2, 0.2)), 0.5, 2.0),
        "eastward_span_north_face": jnp.clip(jnp.exp(math.log(2.0) - 1.3862944 * jax.random.uniform(key_of[5], (NORTHWARD_CELLS, EASTWARD_CELLS), jnp.float32) ** shard_levels(key_of[5], (NORTHWARD_CELLS, EASTWARD_CELLS), ((0, 32), (1, 8)), -0.2, 0.2)), 0.5, 2.0),
        "ocean_flag_east_face": touch_ends((jax.random.randint(key_of[6], (STRATA_COUNT, NORTHWARD_CELLS, EASTWARD_CELLS), 0, 4) < 3).astype(jnp.int32), jax.random.fold_in(key_of[6], 1), 0, 1),
        "ocean_flag_north_face": touch_ends((jax.random.randint(key_of[7], (STRATA_COUNT, NORTHWARD_CELLS, EASTWARD_CELLS), 0, 4) < 3).astype(jnp.int32), jax.random.fold_in(key_of[7], 1), 0, 1),
        "counterpart_across_seam": draw_counterpart_across_seam(jax.random.fold_in(key_of[9], 71), 0),
    }


time_step = 0.2


def interp(a, b, c, d):
    return (7.0 * (b + c) - (a + d)) / 12.0


def advect(umv, vmv, tuv, tvv, rows, cols):
    def cx(field, ro, co):
        return field[..., ro:ro + rows, co:co + cols + 1]

    def ry(field, ro, co):
        return field[..., ro:ro + rows + 1, co:co + cols]

    fut = 0.5 * (cx(tuv, 2, 1) + cx(tuv, 2, 2)) * interp(cx(umv, 2, 0), cx(umv, 2, 1), cx(umv, 2, 2), cx(umv, 2, 3))
    vface = ry(tvv, 1, 2)
    fvf = 0.5 * (vface + ry(tvv, 1, 3)) * interp(ry(umv, 0, 2), ry(umv, 1, 2), ry(umv, 2, 2), ry(umv, 3, 2))
    fuf = 0.5 * (cx(tuv, 2, 1) + cx(tuv, 3, 1)) * interp(cx(vmv, 2, 0), cx(vmv, 2, 1), cx(vmv, 2, 2), cx(vmv, 2, 3))
    fvt = 0.5 * (vface + ry(tvv, 2, 2)) * interp(ry(vmv, 0, 2), ry(vmv, 1, 2), ry(vmv, 2, 2), ry(vmv, 3, 2))
    trend_u = -((fut[..., 1:] - fut[..., :-1]) + (fvf[..., 1:, :] - fvf[..., :-1, :]))
    trend_v = -((fuf[..., 1:] - fuf[..., :-1]) + (fvt[..., 1:, :] - fvt[..., :-1, :]))
    return trend_u, trend_v


def extend(field, counterpart_across_seam):
    north = -field[-2:, :][::-1, :][:, counterpart_across_seam]
    south = jnp.zeros((2, field.shape[1]), jnp.float32)
    padded = jnp.concatenate([south, field, north], axis=0)
    return jnp.concatenate([padded[:, -2:], padded, padded[:, :2]], axis=1)


def reference(eastward_speed_face, northward_speed_face, stratum_extent_east_face, stratum_extent_north_face, northward_span_east_face, eastward_span_north_face, ocean_flag_east_face, ocean_flag_north_face, counterpart_across_seam):
    def stratum_index(items):
        uk, vk, e3uk, e3vk, umk, vmk = items
        um = umk.astype(jnp.float32) * uk
        vm = vmk.astype(jnp.float32) * vk
        volu = northward_span_east_face * e3uk
        volv = eastward_span_north_face * e3vk
        tu = volu * um
        tv = volv * vm
        ext = [extend(f, counterpart_across_seam) for f in (um, vm, tu, tv)]
        trend_u, trend_v = advect(ext[0], ext[1], ext[2], ext[3], um.shape[0], um.shape[1])
        u_new = umk.astype(jnp.float32) * (um + time_step * trend_u / volu)
        v_new = vmk.astype(jnp.float32) * (vm + time_step * trend_v / volv)
        return u_new, v_new

    eastward_speed_next, northward_speed_next = lax.map(stratum_index, (eastward_speed_face, northward_speed_face, stratum_extent_east_face, stratum_extent_north_face, ocean_flag_east_face, ocean_flag_north_face))
    return eastward_speed_next, northward_speed_next
```

```python
import functools

import jax
import jax.numpy as jnp
from jax import lax
from jax.experimental import pallas as pl
from jax.experimental.pallas import tpu as pltpu
from jax.sharding import PartitionSpec as P

MESH = pl.DeviceIdType.MESH
f32 = jnp.float32

FACTOR = 0.2 * 0.5 / 12.0
PAD = 8


def local_copy(src, dst, sem):
    return pltpu.make_async_copy(src, dst, sem)


def kernel(n_lat, n_lon, L, R, C, u, v, eu, ev, wu, wv, mu, mv, seam, ou, ov, *scratch):
    (
        us, vs, eus, evs, wus, wvs, mus, mvs, seams,
        pu, pv, pmu, pmv, peu, pev,
        UM, VM, TU, TV, H,
        SN, SS, SF, EB, WB, CN, CS,
        RS, RN, RW, RE, RCS, RCN, G,
        in_sem, row_sem, send_sem, recv_sem, fold_send, fold_recv,
    ) = scratch
    lat = lax.axis_index("lat")
    lon = lax.axis_index("lon")
    east = lax.rem(lon + 1, n_lon)
    west = lax.rem(lon + n_lon - 1, n_lon)
    has_north = lat < n_lat - 1
    has_south = lat > 0
    pitch = R + 2 * PAD
    blocks = L // 4

    rows = (0, 1, R - 2, R - 1)
    loads = []
    for src, dst in ((u, pu), (v, pv), (mu, pmu), (mv, pmv)):
        for i, r in enumerate(rows):
            loads.append((src.at[:, r, :], dst.at[i]))
    for src, dst in ((eu, peu), (ev, pev)):
        for i, r in enumerate((0, R - 1)):
            loads.append((src.at[:, r, :], dst.at[i]))
    loads.append((wu, wus))
    loads.append((wv, wvs))
    loads.append((seam, seams))
    row_copies = [local_copy(s, d, row_sem.at[i]) for i, (s, d) in enumerate(loads)]
    full_copies = [
        local_copy(s, d, in_sem.at[i])
        for i, (s, d) in enumerate(((u, us), (mu, mus), (v, vs), (mv, mvs), (eu, eus), (ev, evs)))
    ]
    for copy in row_copies:
        copy.start()
    for copy in full_copies:
        copy.start()

    barrier = pltpu.get_barrier_semaphore()

    def greet(a, b):
        pl.semaphore_signal(barrier, inc=1, device_id={"lat": a, "lon": b}, device_id_type=MESH)

    greet(lat, east)
    greet(lat, west)

    @pl.when(has_north)
    def _():
        greet(lat + 1, lon)
        greet(lat + 1, west)

    @pl.when(has_south)
    def _():
        greet(lat - 1, lon)
        greet(lat - 1, east)

    @pl.when(jnp.logical_not(has_north))
    def _():
        for k in range(2, n_lon - 1):
            greet(lat, lax.rem(lon + k, n_lon))

    for copy in row_copies:
        copy.wait()

    lane = lax.broadcasted_iota(jnp.int32, (L, C), 1)
    um0 = pmu[0].astype(f32) * pu[0]
    um1 = pmu[1].astype(f32) * pu[1]
    vm0 = pmv[0].astype(f32) * pv[0]
    vm1 = pmv[1].astype(f32) * pv[1]
    SS[0] = um0
    SS[1] = um1
    SS[2] = vm0
    SS[3] = vm1
    SS[4] = wus[0:1, :] * peu[0] * um0
    SS[5] = wvs[0:1, :] * pev[0] * vm0
    um30 = pmu[2].astype(f32) * pu[2]
    um31 = pmu[3].astype(f32) * pu[3]
    vm30 = pmv[2].astype(f32) * pv[2]
    vm31 = pmv[3].astype(f32) * pv[3]
    tu31 = wus[R - 1 : R, :] * peu[1] * um31
    tv31 = wvs[R - 1 : R, :] * pev[1] * vm31
    SN[0] = um30
    SN[1] = um31
    SN[2] = vm30
    SN[3] = vm31
    SN[4] = tv31
    fill = jnp.zeros((C - L, C), f32)
    CN[...] = jnp.concatenate([tv31, fill], axis=0).T[0:8, :]
    CS[...] = jnp.concatenate([SS[4], fill], axis=0).T[C - 8 : C, :]

    pivot = seams[0] + 1
    tile = pivot // C
    turn = lax.rem(pivot, C)

    @pl.when(jnp.logical_not(has_north))
    def _():
        index = (turn + (2 * C - 1) - lane) & (C - 1)
        for i, plane in enumerate((um31, um30, vm31, vm30, tu31, tv31)):
            SF[i] = -jnp.take_along_axis(plane, index, axis=1)

    @pl.when(has_north & has_south)
    def _():
        pl.semaphore_wait(barrier, 6)

    @pl.when(jnp.logical_not(has_south))
    def _():
        pl.semaphore_wait(barrier, 4)

    @pl.when(jnp.logical_not(has_north))
    def _():
        pl.semaphore_wait(barrier, n_lon + 1)

    def send(src, dst, i, a, b):
        return pltpu.make_async_remote_copy(
            src_ref=src, dst_ref=dst, send_sem=send_sem.at[i], recv_sem=recv_sem.at[i],
            device_id={"lat": a, "lon": b}, device_id_type=MESH,
        )

    to_north = send(SN, RS, 0, lat + 1, lon)
    to_south = send(SS, RN, 1, lat - 1, lon)
    to_east = send(EB, RW, 2, lat, east)
    to_west = send(WB, RE, 3, lat, west)
    to_northwest = send(CN, RCS, 4, lat + 1, west)
    to_southeast = send(CS, RCN, 5, lat - 1, east)

    def fold_copy(k, slot):
        return pltpu.make_async_remote_copy(
            src_ref=SF, dst_ref=G.at[slot], send_sem=fold_send.at[k], recv_sem=fold_recv.at[slot],
            device_id={"lat": lat, "lon": lax.rem(lon + k, n_lon)}, device_id_type=MESH,
        )

    @pl.when(has_north)
    def _():
        to_north.start()
        to_northwest.start()

    @pl.when(has_south)
    def _():
        to_south.start()
        to_southeast.start()

    @pl.when(jnp.logical_not(has_north))
    def _():
        for k in range(1, n_lon):
            fold_copy(k, lon).start()

    for copy in full_copies:
        copy.wait()
    lanes = lax.broadcasted_iota(jnp.int32, (4 * R, C), 1)
    wide_u = jnp.concatenate([wus[...]] * 4, axis=0)
    wide_v = jnp.concatenate([wvs[...]] * 4, axis=0)

    def pack(g, carry):
        def whole(ref):
            return ref[pl.ds(g * 4, 4)].reshape(4 * R, C)

        um = whole(mus).astype(f32) * whole(us)
        vm = whole(mvs).astype(f32) * whole(vs)
        tu = wide_u * whole(eus) * um
        tv = wide_v * whole(evs) * vm
        for i in range(4):
            to = pl.ds(pl.multiple_of((g * 4 + i) * pitch + PAD, 8), R)
            UM[to, :] = um[i * R : (i + 1) * R]
            VM[to, :] = vm[i * R : (i + 1) * R]
            TU[to, :] = tu[i * R : (i + 1) * R]
            TV[to, :] = tv[i * R : (i + 1) * R]
        both = jnp.where((lanes >= 2) & (lanes <= 5), pltpu.roll(vm, 4, 1), um)
        both = jnp.where((lanes == 6) | (lanes == 7), pltpu.roll(tu, 7, 1), both)
        both = jnp.where(lanes == C - 3, pltpu.roll(tv, C - 3, 1), both)
        turned = both.T
        for f, r in enumerate((C - 2, C - 1, 2, 3, 6)):
            EB[f, pl.ds(g, 1), :] = turned[r : r + 1, :]
        for f, r in enumerate((0, 1, 4, 5, 7, C - 3)):
            WB[f, pl.ds(g, 1), :] = turned[r : r + 1, :]
        return carry

    lax.fori_loop(0, blocks, pack, 0)
    to_east.start()
    to_west.start()

    to_east.wait_recv()
    to_west.wait_recv()
    sub = lax.broadcasted_iota(jnp.int32, (8, C), 0)

    def stacked(parts):
        out = jnp.zeros((8, C), f32)
        for r, row in parts:
            out = jnp.where(sub == r, jnp.broadcast_to(row, (8, C)), out)
        return out

    def unpack(g, carry):
        w = [RW[f, pl.ds(g, 1), :] for f in range(5)]
        e = [RE[f, pl.ds(g, 1), :] for f in range(6)]
        first = stacked(list(enumerate((e[0], e[1], w[2], w[3], e[2], e[3], w[4], e[4]))))
        last = stacked(((5, e[5]), (6, w[0]), (7, w[1])))
        turned = jnp.concatenate([first, jnp.zeros((C - 16, C), f32), last], axis=0).T
        for i in range(4):
            to = pl.ds(pl.multiple_of((g * 4 + i) * pitch + PAD, 8), R)
            H[to, :] = turned[i * R : (i + 1) * R]
        return carry

    lax.fori_loop(0, blocks, unpack, 0)

    def row_of(r):
        return pl.ds(PAD + r, L, stride=pitch)

    @pl.when(has_south)
    def _():
        to_north.wait_recv()
        to_northwest.wait_recv()
        UM[row_of(-2), :] = RS[0]
        UM[row_of(-1), :] = RS[1]
        VM[row_of(-2), :] = RS[2]
        VM[row_of(-1), :] = RS[3]
        TV[row_of(-1), :] = RS[4]
        last = stacked(((5, RCS[0:1, :]),))
        H[row_of(-1), :] = jnp.concatenate([jnp.zeros((C - 8, C), f32), last], axis=0).T[0:L, :]

    @pl.when(jnp.logical_not(has_south))
    def _():
        zero = jnp.zeros((L, C), f32)
        UM[row_of(-2), :] = zero
        UM[row_of(-1), :] = zero
        VM[row_of(-2), :] = zero
        VM[row_of(-1), :] = zero
        TV[row_of(-1), :] = zero
        H[row_of(-1), :] = zero

    north = ((UM, 0), (UM, 1), (VM, 0), (VM, 1), (TU, 0), (TV, 0))

    @pl.when(has_north)
    def _():
        to_south.wait_recv()
        to_southeast.wait_recv()
        for i, (field, r) in enumerate(north):
            field[row_of(R + r), :] = RN[i]
        first = stacked(((6, RCN[7:8, :]),))
        H[row_of(R), :] = jnp.concatenate([first, jnp.zeros((C - 8, C), f32)], axis=0).T[0:L, :]

    @pl.when(jnp.logical_not(has_north))
    def _():
        for k in range(1, n_lon):
            fold_copy(k, lax.rem(lon + n_lon - k, n_lon)).wait_recv()
        G[lon] = SF[...]
        low = lax.rem(tile - lon + 2 * n_lon, n_lon)
        high = lax.rem(tile - lon + 2 * n_lon - 1, n_lon)
        for i, (field, r) in enumerate(north):
            field[row_of(R + r), :] = jnp.where(lane < turn, G[low, i], G[high, i])
        H[row_of(R), :] = pltpu.roll(G[low, 4], 7, 1)

    col = lax.broadcasted_iota(jnp.int32, (8, C), 1)

    def left1(x, h):
        return pltpu.roll(jnp.where(col == C - 1, h, x), 1, 1)

    def left2(x, h):
        return pltpu.roll(jnp.where(col >= C - 2, h, x), 2, 1)

    def right1(x, h):
        return pltpu.roll(jnp.where(col == 0, h, x), C - 1, 1)

    def right2(x, h):
        return pltpu.roll(jnp.where(col <= 1, h, x), C - 2, 1)

    def q(a, b, c, d):
        return 7.0 * (b + c) - (a + d)

    def level(k, carry):
        for b in range(R // 8):
            base = pl.multiple_of(k * pitch + PAD + 8 * b, 8)
            at = pl.ds(8 * b, 8)

            def get(ref, o):
                return ref[pl.ds(base + o, 8), :]

            h0, hp, hm = get(H, 0), get(H, 1), get(H, -1)
            um2, um1, u0, up1, up2 = (get(UM, o) for o in (-2, -1, 0, 1, 2))
            vm2, vm1, v0, vp1, vp2 = (get(VM, o) for o in (-2, -1, 0, 1, 2))
            t0, t1 = get(TU, 0), get(TU, 1)
            sm, s0, sp = get(TV, -1), get(TV, 0), get(TV, 1)
            volu = wus[8 * b : 8 * b + 8, :] * eus[k, at, :]
            volv = wvs[8 * b : 8 * b + 8, :] * evs[k, at, :]

            a1, a2, b1, b2 = left1(u0, h0), left2(u0, h0), right1(u0, h0), right2(u0, h0)
            ht = pltpu.roll(h0, C - 7, 1)
            htp = pltpu.roll(hp, C - 7, 1)
            tl, tr = left1(t0, ht), right1(t0, ht)
            du = (t0 + tr) * q(a1, u0, b1, b2) - (tl + t0) * q(a2, a1, u0, b1)
            sr = right1(s0, pltpu.roll(h0, 3, 1))
            smr = right1(sm, pltpu.roll(hm, 3, 1))
            du = du + ((s0 + sr) * q(um1, u0, up1, up2) - (sm + smr) * q(um2, um1, u0, up1))
            ou[k, at, :] = mus[k, at, :].astype(f32) * (u0 - FACTOR * du / volu)

            hv = pltpu.roll(h0, C - 4, 1)
            c1, c2, d1, d2 = left1(v0, hv), left2(v0, hv), right1(v0, hv), right2(v0, hv)
            ts = t0 + t1
            tsl = left1(ts, ht + htp)
            dv = ts * q(c1, v0, d1, d2) - tsl * q(c2, c1, v0, d1)
            dv = dv + ((s0 + sp) * q(vm1, v0, vp1, vp2) - (sm + s0) * q(vm2, vm1, v0, vp1))
            ov[k, at, :] = mvs[k, at, :].astype(f32) * (v0 - FACTOR * dv / volv)
        return carry

    lax.fori_loop(0, L, level, 0)

    to_east.wait_send()
    to_west.wait_send()

    @pl.when(has_north)
    def _():
        to_north.wait_send()
        to_northwest.wait_send()

    @pl.when(has_south)
    def _():
        to_south.wait_send()
        to_southeast.wait_send()

    @pl.when(jnp.logical_not(has_north))
    def _():
        for k in range(1, n_lon):
            fold_copy(k, lon).wait_send()


def local(n_lat, n_lon, u, v, eu, ev, wu, wv, mu, mv, seam):
    L, R, C = u.shape
    cube = (L, R, C)
    pitch = R + 2 * PAD
    vm = pltpu.VMEM
    scratch = (
        [vm(cube, f32)] * 4
        + [vm((R, C), f32)] * 2
        + [vm(cube, jnp.int32)] * 2
        + [pltpu.SMEM(seam.shape, jnp.int32)]
        + [vm((4, L, C), f32)] * 2
        + [vm((4, L, C), jnp.int32)] * 2
        + [vm((2, L, C), f32)] * 2
        + [vm((L * pitch, C), f32)] * 5
        + [vm((5, L, C), f32), vm((6, L, C), f32), vm((6, L, C), f32)]
        + [vm((5, L // 4, C), f32), vm((6, L // 4, C), f32)]
        + [vm((8, C), f32)] * 2
        + [vm((5, L, C), f32), vm((6, L, C), f32)]
        + [vm((5, L // 4, C), f32), vm((6, L // 4, C), f32)]
        + [vm((8, C), f32)] * 2
        + [vm((n_lon, 6, L, C), f32)]
        + [
            pltpu.SemaphoreType.DMA((6,)),
            pltpu.SemaphoreType.DMA((23,)),
            pltpu.SemaphoreType.DMA((6,)),
            pltpu.SemaphoreType.DMA((6,)),
            pltpu.SemaphoreType.DMA((n_lon,)),
            pltpu.SemaphoreType.DMA((n_lon,)),
        ]
    )
    anywhere = pl.BlockSpec(memory_space=pltpu.HBM)
    nu, nv = pl.pallas_call(
        functools.partial(kernel, n_lat, n_lon, L, R, C),
        out_shape=[jax.ShapeDtypeStruct(cube, f32)] * 2,
        in_specs=[anywhere] * 9,
        out_specs=[pl.BlockSpec(memory_space=pltpu.VMEM)] * 2,
        scratch_shapes=scratch,
        compiler_params=pltpu.CompilerParams(
            collective_id=0, has_side_effects=True, vmem_limit_bytes=60 * 1024 * 1024
        ),
    )(u, v, eu, ev, wu, wv, mu, mv, seam)
    return nu, nv


def solution(mesh):
    n_lat, n_lon = mesh.shape["lat"], mesh.shape["lon"]
    cube = P(None, "lat", "lon")
    flat = P("lat", "lon")
    return jax.shard_map(
        functools.partial(local, n_lat, n_lon),
        mesh=mesh,
        in_specs=(cube, cube, cube, cube, flat, flat, cube, cube, P()),
        out_specs=(cube, cube),
        check_vma=False,
    )
```

```python
import functools

import jax
import jax.numpy as jnp
from jax import lax
from jax.experimental import pallas as pl
from jax.experimental.pallas import tpu as pltpu
from jax.sharding import PartitionSpec as P

MESH = pl.DeviceIdType.MESH
f32 = jnp.float32

FACTOR = 0.2 * 0.5 / 12.0
PAD = 8


def local_copy(src, dst, sem):
    return pltpu.make_async_copy(src, dst, sem)


def kernel(n_lat, n_lon, L, R, C, tile, u, v, eu, ev, wu, wv, mu, mv, seam, ou, ov, *scratch):
    (
        us, vs, eus, evs, wus, wvs, mus, mvs, seams,
        pu, pv, pmu, pmv, peu, pev,
        UM, VM, TU, TV, H,
        SN, SS, SF, EB, WB, CN, CS,
        RS, RN, RW, RE, RCS, RCN, G,
        in_sem, row_sem, send_sem, recv_sem, fold_send, fold_recv,
    ) = scratch
    lat = lax.axis_index("lat")
    lon = lax.axis_index("lon")
    east = lax.rem(lon + 1, n_lon)
    west = lax.rem(lon + n_lon - 1, n_lon)
    has_north = lat < n_lat - 1
    has_south = lat > 0
    pitch = R + 2 * PAD
    blocks = L // 4

    rows = (0, 1, R - 2, R - 1)
    loads = []
    for src, dst in ((u, pu), (v, pv), (mu, pmu), (mv, pmv)):
        for i, r in enumerate(rows):
            loads.append((src.at[:, r, :], dst.at[i]))
    for src, dst in ((eu, peu), (ev, pev)):
        for i, r in enumerate((0, R - 1)):
            loads.append((src.at[:, r, :], dst.at[i]))
    loads.append((wu, wus))
    loads.append((wv, wvs))
    loads.append((seam, seams))
    row_copies = [local_copy(s, d, row_sem.at[i]) for i, (s, d) in enumerate(loads)]
    full_copies = [
        local_copy(s, d, in_sem.at[i])
        for i, (s, d) in enumerate(((u, us), (mu, mus), (v, vs), (mv, mvs), (eu, eus), (ev, evs)))
    ]
    for copy in row_copies:
        copy.start()
    for copy in full_copies:
        copy.start()

    barrier = pltpu.get_barrier_semaphore()

    def greet(a, b):
        pl.semaphore_signal(barrier, inc=1, device_id={"lat": a, "lon": b}, device_id_type=MESH)

    greet(lat, east)
    greet(lat, west)

    @pl.when(has_north)
    def _():
        greet(lat + 1, lon)
        greet(lat + 1, west)

    @pl.when(has_south)
    def _():
        greet(lat - 1, lon)
        greet(lat - 1, east)

    @pl.when(jnp.logical_not(has_north))
    def _():
        for k in range(2, n_lon - 1):
            greet(lat, lax.rem(lon + k, n_lon))

    for copy in row_copies:
        copy.wait()

    lane = lax.broadcasted_iota(jnp.int32, (L, C), 1)
    um0 = pmu[0].astype(f32) * pu[0]
    um1 = pmu[1].astype(f32) * pu[1]
    vm0 = pmv[0].astype(f32) * pv[0]
    vm1 = pmv[1].astype(f32) * pv[1]
    SS[0] = um0
    SS[1] = um1
    SS[2] = vm0
    SS[3] = vm1
    SS[4] = wus[0:1, :] * peu[0] * um0
    SS[5] = wvs[0:1, :] * pev[0] * vm0
    um30 = pmu[2].astype(f32) * pu[2]
    um31 = pmu[3].astype(f32) * pu[3]
    vm30 = pmv[2].astype(f32) * pv[2]
    vm31 = pmv[3].astype(f32) * pv[3]
    tu31 = wus[R - 1 : R, :] * peu[1] * um31
    tv31 = wvs[R - 1 : R, :] * pev[1] * vm31
    SN[0] = um30
    SN[1] = um31
    SN[2] = vm30
    SN[3] = vm31
    SN[4] = tv31
    fill = jnp.zeros((C - L, C), f32)
    CN[...] = jnp.concatenate([tv31, fill], axis=0).T[0:8, :]
    CS[...] = jnp.concatenate([SS[4], fill], axis=0).T[C - 8 : C, :]

    turn = lax.rem(seams[0] + 1, C)
    fold_peers = (lax.rem(tile + n_lon - lon, n_lon), lax.rem(tile + 2 * n_lon - 1 - lon, n_lon))

    @pl.when(jnp.logical_not(has_north))
    def _():
        index = (turn + (2 * C - 1) - lane) & (C - 1)
        for i, plane in enumerate((um31, um30, vm31, vm30, tu31, tv31)):
            SF[i] = -jnp.take_along_axis(plane, index, axis=1)

    @pl.when(has_north & has_south)
    def _():
        pl.semaphore_wait(barrier, 6)

    @pl.when(jnp.logical_not(has_south))
    def _():
        pl.semaphore_wait(barrier, 4)

    @pl.when(jnp.logical_not(has_north))
    def _():
        pl.semaphore_wait(barrier, n_lon + 1)

    def send(src, dst, i, a, b):
        return pltpu.make_async_remote_copy(
            src_ref=src, dst_ref=dst, send_sem=send_sem.at[i], recv_sem=recv_sem.at[i],
            device_id={"lat": a, "lon": b}, device_id_type=MESH,
        )

    to_north = send(SN, RS, 0, lat + 1, lon)
    to_south = send(SS, RN, 1, lat - 1, lon)
    to_east = send(EB, RW, 2, lat, east)
    to_west = send(WB, RE, 3, lat, west)
    to_northwest = send(CN, RCS, 4, lat + 1, west)
    to_southeast = send(CS, RCN, 5, lat - 1, east)

    def fold_copy(slot):
        return pltpu.make_async_remote_copy(
            src_ref=SF, dst_ref=G.at[slot], send_sem=fold_send.at[slot], recv_sem=fold_recv.at[slot],
            device_id={"lat": lat, "lon": fold_peers[slot]}, device_id_type=MESH,
        )

    def each_fold(act, own=None):
        for slot in range(2):
            mine = fold_peers[slot] == lon

            @pl.when(jnp.logical_not(has_north | mine))
            def _(slot=slot):
                act(slot)

            if own is not None:

                @pl.when(jnp.logical_not(has_north) & mine)
                def _(slot=slot):
                    own(slot)

    @pl.when(has_north)
    def _():
        to_north.start()
        to_northwest.start()

    @pl.when(has_south)
    def _():
        to_south.start()
        to_southeast.start()

    each_fold(lambda slot: fold_copy(slot).start())

    for copy in full_copies:
        copy.wait()
    lanes = lax.broadcasted_iota(jnp.int32, (4 * R, C), 1)
    wide_u = jnp.concatenate([wus[...]] * 4, axis=0)
    wide_v = jnp.concatenate([wvs[...]] * 4, axis=0)

    def pack(g, carry):
        def whole(ref):
            return ref[pl.ds(g * 4, 4)].reshape(4 * R, C)

        um = whole(mus).astype(f32) * whole(us)
        vm = whole(mvs).astype(f32) * whole(vs)
        tu = wide_u * whole(eus) * um
        tv = wide_v * whole(evs) * vm
        for i in range(4):
            to = pl.ds(pl.multiple_of((g * 4 + i) * pitch + PAD, 8), R)
            UM[to, :] = um[i * R : (i + 1) * R]
            VM[to, :] = vm[i * R : (i + 1) * R]
            TU[to, :] = tu[i * R : (i + 1) * R]
            TV[to, :] = tv[i * R : (i + 1) * R]
        both = jnp.where((lanes >= 2) & (lanes <= 5), pltpu.roll(vm, 4, 1), um)
        both = jnp.where((lanes == 6) | (lanes == 7), pltpu.roll(tu, 7, 1), both)
        both = jnp.where(lanes == C - 3, pltpu.roll(tv, C - 3, 1), both)
        turned = both.T
        for f, r in enumerate((C - 2, C - 1, 2, 3, 6)):
            EB[f, pl.ds(g, 1), :] = turned[r : r + 1, :]
        for f, r in enumerate((0, 1, 4, 5, 7, C - 3)):
            WB[f, pl.ds(g, 1), :] = turned[r : r + 1, :]
        return carry

    lax.fori_loop(0, blocks, pack, 0)
    to_east.start()
    to_west.start()

    to_east.wait_recv()
    to_west.wait_recv()
    sub = lax.broadcasted_iota(jnp.int32, (8, C), 0)

    def stacked(parts):
        out = jnp.zeros((8, C), f32)
        for r, row in parts:
            out = jnp.where(sub == r, jnp.broadcast_to(row, (8, C)), out)
        return out

    def unpack(g, carry):
        w = [RW[f, pl.ds(g, 1), :] for f in range(5)]
        e = [RE[f, pl.ds(g, 1), :] for f in range(6)]
        first = stacked(list(enumerate((e[0], e[1], w[2], w[3], e[2], e[3], w[4], e[4]))))
        last = stacked(((5, e[5]), (6, w[0]), (7, w[1])))
        turned = jnp.concatenate([first, jnp.zeros((C - 16, C), f32), last], axis=0).T
        for i in range(4):
            to = pl.ds(pl.multiple_of((g * 4 + i) * pitch + PAD, 8), R)
            H[to, :] = turned[i * R : (i + 1) * R]
        return carry

    lax.fori_loop(0, blocks, unpack, 0)

    def row_of(r):
        return pl.ds(PAD + r, L, stride=pitch)

    @pl.when(has_south)
    def _():
        to_north.wait_recv()
        to_northwest.wait_recv()
        UM[row_of(-2), :] = RS[0]
        UM[row_of(-1), :] = RS[1]
        VM[row_of(-2), :] = RS[2]
        VM[row_of(-1), :] = RS[3]
        TV[row_of(-1), :] = RS[4]
        last = stacked(((5, RCS[0:1, :]),))
        H[row_of(-1), :] = jnp.concatenate([jnp.zeros((C - 8, C), f32), last], axis=0).T[0:L, :]

    @pl.when(jnp.logical_not(has_south))
    def _():
        zero = jnp.zeros((L, C), f32)
        UM[row_of(-2), :] = zero
        UM[row_of(-1), :] = zero
        VM[row_of(-2), :] = zero
        VM[row_of(-1), :] = zero
        TV[row_of(-1), :] = zero
        H[row_of(-1), :] = zero

    north = ((UM, 0), (UM, 1), (VM, 0), (VM, 1), (TU, 0), (TV, 0))

    @pl.when(has_north)
    def _():
        to_south.wait_recv()
        to_southeast.wait_recv()
        for i, (field, r) in enumerate(north):
            field[row_of(R + r), :] = RN[i]
        first = stacked(((6, RCN[7:8, :]),))
        H[row_of(R), :] = jnp.concatenate([first, jnp.zeros((C - 8, C), f32)], axis=0).T[0:L, :]

    def own_fold(slot):
        G[slot] = SF[...]

    each_fold(lambda slot: fold_copy(slot).wait_recv(), own_fold)

    @pl.when(jnp.logical_not(has_north))
    def _():
        for i, (field, r) in enumerate(north):
            field[row_of(R + r), :] = jnp.where(lane < turn, G[0, i], G[1, i])
        H[row_of(R), :] = pltpu.roll(G[0, 4], 7, 1)

    col = lax.broadcasted_iota(jnp.int32, (8, C), 1)

    def left1(x, h):
        return pltpu.roll(jnp.where(col == C - 1, h, x), 1, 1)

    def left2(x, h):
        return pltpu.roll(jnp.where(col >= C - 2, h, x), 2, 1)

    def right1(x, h):
        return pltpu.roll(jnp.where(col == 0, h, x), C - 1, 1)

    def right2(x, h):
        return pltpu.roll(jnp.where(col <= 1, h, x), C - 2, 1)

    def q(a, b, c, d):
        return 7.0 * (b + c) - (a + d)

    def level(k, carry):
        for b in range(R // 8):
            base = pl.multiple_of(k * pitch + PAD + 8 * b, 8)
            at = pl.ds(8 * b, 8)

            def get(ref, o):
                return ref[pl.ds(base + o, 8), :]

            h0, hp, hm = get(H, 0), get(H, 1), get(H, -1)
            um2, um1, u0, up1, up2 = (get(UM, o) for o in (-2, -1, 0, 1, 2))
            vm2, vm1, v0, vp1, vp2 = (get(VM, o) for o in (-2, -1, 0, 1, 2))
            t0, t1 = get(TU, 0), get(TU, 1)
            sm, s0, sp = get(TV, -1), get(TV, 0), get(TV, 1)
            volu = wus[8 * b : 8 * b + 8, :] * eus[k, at, :]
            volv = wvs[8 * b : 8 * b + 8, :] * evs[k, at, :]

            a1, a2, b1, b2 = left1(u0, h0), left2(u0, h0), right1(u0, h0), right2(u0, h0)
            ht = pltpu.roll(h0, C - 7, 1)
            htp = pltpu.roll(hp, C - 7, 1)
            tl, tr = left1(t0, ht), right1(t0, ht)
            du = (t0 + tr) * q(a1, u0, b1, b2) - (tl + t0) * q(a2, a1, u0, b1)
            sr = right1(s0, pltpu.roll(h0, 3, 1))
            smr = right1(sm, pltpu.roll(hm, 3, 1))
            du = du + ((s0 + sr) * q(um1, u0, up1, up2) - (sm + smr) * q(um2, um1, u0, up1))
            ou[k, at, :] = mus[k, at, :].astype(f32) * (u0 - FACTOR * du / volu)

            hv = pltpu.roll(h0, C - 4, 1)
            c1, c2, d1, d2 = left1(v0, hv), left2(v0, hv), right1(v0, hv), right2(v0, hv)
            ts = t0 + t1
            tsl = left1(ts, ht + htp)
            dv = ts * q(c1, v0, d1, d2) - tsl * q(c2, c1, v0, d1)
            dv = dv + ((s0 + sp) * q(vm1, v0, vp1, vp2) - (sm + s0) * q(vm2, vm1, v0, vp1))
            ov[k, at, :] = mvs[k, at, :].astype(f32) * (v0 - FACTOR * dv / volv)
        return carry

    lax.fori_loop(0, L, level, 0)

    to_east.wait_send()
    to_west.wait_send()

    @pl.when(has_north)
    def _():
        to_north.wait_send()
        to_northwest.wait_send()

    @pl.when(has_south)
    def _():
        to_south.wait_send()
        to_southeast.wait_send()

    each_fold(lambda slot: fold_copy(slot).wait_send())


def local(n_lat, n_lon, u, v, eu, ev, wu, wv, mu, mv, seam):
    L, R, C = u.shape
    cube = (L, R, C)
    pitch = R + 2 * PAD
    vm = pltpu.VMEM
    scratch = (
        [vm(cube, f32)] * 4
        + [vm((R, C), f32)] * 2
        + [vm(cube, jnp.int32)] * 2
        + [pltpu.SMEM(seam.shape, jnp.int32)]
        + [vm((4, L, C), f32)] * 2
        + [vm((4, L, C), jnp.int32)] * 2
        + [vm((2, L, C), f32)] * 2
        + [vm((L * pitch, C), f32)] * 5
        + [vm((5, L, C), f32), vm((6, L, C), f32), vm((6, L, C), f32)]
        + [vm((5, L // 4, C), f32), vm((6, L // 4, C), f32)]
        + [vm((8, C), f32)] * 2
        + [vm((5, L, C), f32), vm((6, L, C), f32)]
        + [vm((5, L // 4, C), f32), vm((6, L // 4, C), f32)]
        + [vm((8, C), f32)] * 2
        + [vm((2, 6, L, C), f32)]
        + [
            pltpu.SemaphoreType.DMA((6,)),
            pltpu.SemaphoreType.DMA((23,)),
            pltpu.SemaphoreType.DMA((6,)),
            pltpu.SemaphoreType.DMA((6,)),
            pltpu.SemaphoreType.DMA((2,)),
            pltpu.SemaphoreType.DMA((2,)),
        ]
    )
    anywhere = pl.BlockSpec(memory_space=pltpu.HBM)

    def step(tile, *operands):
        return pl.pallas_call(
            functools.partial(kernel, n_lat, n_lon, L, R, C, tile),
            out_shape=[jax.ShapeDtypeStruct(cube, f32)] * 2,
            in_specs=[anywhere] * 9,
            out_specs=[pl.BlockSpec(memory_space=pltpu.VMEM)] * 2,
            scratch_shapes=scratch,
            compiler_params=pltpu.CompilerParams(
                collective_id=tile, has_side_effects=True, vmem_limit_bytes=32 * 1024 * 1024
            ),
        )(*(pltpu.with_memory_space_constraint(x, pltpu.HBM) for x in operands))

    tile = lax.rem((seam[0] + 1) // C, n_lon)
    branches = [functools.partial(step, t) for t in range(n_lon)]
    return tuple(lax.switch(tile, branches, u, v, eu, ev, wu, wv, mu, mv, seam))


def solution(mesh):
    n_lat, n_lon = mesh.shape["lat"], mesh.shape["lon"]
    cube = P(None, "lat", "lon")
    flat = P("lat", "lon")
    return jax.shard_map(
        functools.partial(local, n_lat, n_lon),
        mesh=mesh,
        in_specs=(cube, cube, cube, cube, flat, flat, cube, cube, P()),
        out_specs=(cube, cube),
        check_vma=False,
    )
```

```python
import functools

import jax
import jax.numpy as jnp
from jax import lax
from jax.experimental import pallas as pl
from jax.experimental.pallas import tpu as pltpu
from jax.sharding import PartitionSpec as P

MESH = pl.DeviceIdType.MESH
f32 = jnp.float32

FACTOR = 0.2 * 0.5 / 12.0


U_COLS = {126: 0, 127: 1, 0: 5, 1: 6, 124: 11, 125: 12, 2: 13, 3: 14}
V_COLS = {126: 2, 127: 3, 0: 7, 1: 8, 124: 15, 125: 16, 2: 17, 3: 18}
T_COLS = {127: 4, 0: 9, 125: 19, 126: 20, 1: 21, 2: 22}
S_COLS = {0: 10, 126: 23, 127: 24, 1: 25, 2: 26}
OWN = 27
U_AT, V_AT, T_AT, S_AT = 0, 8, 15, 20


def q(a, b, c, d):
    return 7.0 * (b + c) - (a + d)


def roll(x, shift):
    return pltpu.roll(x, shift % x.shape[1], 1)


def kernel(n_lat, n_lon, L, R, C, LC, tile, u, v, eu, ev, wu, wv, mu, mv, seam, ou, ov, *scratch):
    (
        us, vs, eus, evs, wus, wvs, mus, mvs, seams,
        pu, pv, pmu, pmv, peu, pev,
        UM, VM, TU, TV, TS,
        SN, SS, SF, CN, CS,
        RS, RN, RCS, RCN, G, KS, KN,
        TO, TC, TX, RW, RE, HP,
        in_sem, row_sem, send_sem, recv_sem, fold_send, fold_recv, lon_send, lon_recv,
    ) = scratch
    lat = lax.axis_index("lat")
    lon = lax.axis_index("lon")
    east = lax.rem(lon + 1, n_lon)
    west = lax.rem(lon + n_lon - 1, n_lon)
    has_north = lat < n_lat - 1
    has_south = lat > 0
    pitch = R + 8
    chunks = L // LC
    GB = LC // 4

    rows = (0, 1, R - 2, R - 1)
    loads = [(wu, wus), (wv, wvs), (seam, seams)]
    for src, dst in ((u, pu), (mu, pmu), (v, pv), (mv, pmv), (eu, peu), (ev, pev)):
        for i, r in enumerate(rows):
            loads.append((src.at[:, r, :], dst.at[i]))
    row_copies = [pltpu.make_async_copy(s, d, row_sem.at[i]) for i, (s, d) in enumerate(loads)]
    fields = ((u, us), (mu, mus), (v, vs), (mv, mvs), (eu, eus), (ev, evs))
    full_copies = [
        [
            pltpu.make_async_copy(s.at[pl.ds(c * LC, LC)], d.at[pl.ds(c * LC, LC)], in_sem.at[c, i])
            for i, (s, d) in enumerate(fields)
        ]
        for c in range(chunks)
    ]
    for copy in row_copies:
        copy.start()
    for group in full_copies:
        for copy in group:
            copy.start()

    barrier = pltpu.get_barrier_semaphore()

    def greet(a, b):
        pl.semaphore_signal(barrier, inc=1, device_id={"lat": a, "lon": b}, device_id_type=MESH)

    greet(lat, east)
    greet(lat, west)

    @pl.when(has_north)
    def _():
        greet(lat + 1, lon)
        greet(lat + 1, west)

    @pl.when(has_south)
    def _():
        greet(lat - 1, lon)
        greet(lat - 1, east)

    @pl.when(jnp.logical_not(has_north))
    def _():
        for k in range(2, n_lon - 1):
            greet(lat, lax.rem(lon + k, n_lon))

    for copy in row_copies:
        copy.wait()

    lane = lax.broadcasted_iota(jnp.int32, (L, C), 1)
    um0 = pmu[0].astype(f32) * pu[0]
    um1 = pmu[1].astype(f32) * pu[1]
    vm0 = pmv[0].astype(f32) * pv[0]
    vm1 = pmv[1].astype(f32) * pv[1]
    tu0 = wus[0:1, :] * peu[0] * um0
    SS[0] = um0
    SS[1] = um1
    SS[2] = vm0
    SS[3] = vm1
    SS[4] = tu0
    SS[5] = wvs[0:1, :] * pev[0] * vm0
    um30 = pmu[2].astype(f32) * pu[2]
    um31 = pmu[3].astype(f32) * pu[3]
    vm30 = pmv[2].astype(f32) * pv[2]
    vm31 = pmv[3].astype(f32) * pv[3]
    tv31 = wvs[R - 1 : R, :] * pev[3] * vm31
    SN[0] = um30
    SN[1] = um31
    SN[2] = vm30
    SN[3] = vm31
    SN[4] = tv31
    fill = jnp.zeros((C - L, C), f32)
    CN[...] = jnp.concatenate([tv31, fill], axis=0).T[0:8, :]
    CS[...] = jnp.concatenate([tu0, fill], axis=0).T[C - 8 : C, :]

    turn = lax.rem(seams[0] + 1, C)
    fold_peers = (lax.rem(tile + n_lon - lon, n_lon), lax.rem(tile + 2 * n_lon - 1 - lon, n_lon))

    @pl.when(jnp.logical_not(has_north))
    def _():
        index = (turn + (2 * C - 1) - lane) & (C - 1)
        tu31 = wus[R - 1 : R, :] * peu[3] * um31
        for i, plane in enumerate((um31, um30, vm31, vm30, tu31, tv31)):
            SF[i] = -jnp.take_along_axis(plane, index, axis=1)

    @pl.when(has_north & has_south)
    def _():
        pl.semaphore_wait(barrier, 6)

    @pl.when(jnp.logical_not(has_south))
    def _():
        pl.semaphore_wait(barrier, 4)

    @pl.when(jnp.logical_not(has_north))
    def _():
        pl.semaphore_wait(barrier, n_lon + 1)

    def send(src, dst, i, a, b):
        return pltpu.make_async_remote_copy(
            src_ref=src, dst_ref=dst, send_sem=send_sem.at[i], recv_sem=recv_sem.at[i],
            device_id={"lat": a, "lon": b}, device_id_type=MESH,
        )

    def send_columns(src, dst, c, i, b):
        return pltpu.make_async_remote_copy(
            src_ref=src, dst_ref=dst, send_sem=lon_send.at[c, i], recv_sem=lon_recv.at[c, i],
            device_id={"lat": lat, "lon": b}, device_id_type=MESH,
        )

    to_north = send(SN, RS, 0, lat + 1, lon)
    to_south = send(SS, RN, 1, lat - 1, lon)
    to_northwest = send(CN, RCS, 2, lat + 1, west)
    to_southeast = send(CS, RCN, 3, lat - 1, east)
    to_east = [send_columns(TO.at[c, 0:5], RW.at[c], c, 0, east) for c in range(chunks)]
    to_west = [send_columns(TO.at[c, 5:11], RE.at[c], c, 1, west) for c in range(chunks)]

    def fold_copy(slot):
        return pltpu.make_async_remote_copy(
            src_ref=SF, dst_ref=G.at[slot], send_sem=fold_send.at[slot], recv_sem=fold_recv.at[slot],
            device_id={"lat": lat, "lon": fold_peers[slot]}, device_id_type=MESH,
        )

    def each_fold(act, own=None):
        for slot in range(2):
            mine = fold_peers[slot] == lon

            @pl.when(jnp.logical_not(has_north | mine))
            def _(slot=slot):
                act(slot)

            if own is not None:

                @pl.when(jnp.logical_not(has_north) & mine)
                def _(slot=slot):
                    own(slot)

    @pl.when(has_north)
    def _():
        to_north.start()
        to_northwest.start()

    @pl.when(has_south)
    def _():
        to_south.start()
        to_southeast.start()

    each_fold(lambda slot: fold_copy(slot).start())

    lanes = lax.broadcasted_iota(jnp.int32, (4 * R, C), 1)
    wide_u = jnp.concatenate([wus[...]] * 4, axis=0)
    wide_v = jnp.concatenate([wvs[...]] * 4, axis=0)

    def level_rows(k, o=0):
        return pl.ds(pl.multiple_of(k * pitch + 8, 8) + o, R)

    def pack(c, g):
        first = c * LC + 4 * g

        def whole(ref):
            return ref[pl.ds(first, 4)].reshape(4 * R, C)

        um = whole(mus).astype(f32) * whole(us)
        vm = whole(mvs).astype(f32) * whole(vs)
        tu = wide_u * whole(eus) * um
        tv = wide_v * whole(evs) * vm
        for i in range(4):
            part = slice(i * R, (i + 1) * R)
            to = level_rows(first + i)
            UM[to, :] = um[part]
            VM[to, :] = vm[part]
            TU[to, :] = tu[part]
            TV[to, :] = tv[part]
        both = jnp.where((lanes >= 4) & (lanes <= 11), roll(vm, V_AT), um)
        both = jnp.where((lanes >= 12) & (lanes <= 17), roll(tu, T_AT), both)
        both = jnp.where((lanes >= 18) & (lanes <= 22), roll(tv, S_AT), both)
        turned = both.T
        for at, columns in ((U_AT, U_COLS), (V_AT, V_COLS), (T_AT, T_COLS), (S_AT, S_COLS)):
            for column, row in columns.items():
                r = (column + at) % C
                TO[c, row, pl.ds(g, 1), :] = turned[r : r + 1, :]

    per = 3 if GB % 3 == 0 else 2
    for c in range(chunks):
        for copy in full_copies[c]:
            copy.wait()

        def some(h, carry, c=c):
            for i in range(per):
                pack(c, h * per + i)
            return carry

        lax.fori_loop(0, GB // per, some, 0)
        to_east[c].start()
        to_west[c].start()

    def sums(k, carry):
        at = pl.ds(pl.multiple_of(k * pitch * 4 + 8, 8), pitch * 4)
        tv = TV[at, :]
        TS[at, :] = tv + roll(tv, -1)
        return carry

    lax.fori_loop(0, L // 4, sums, 0)

    at_lane = lanes[0 : 4 * R]

    def step(k):
        def get(ref, o):
            return ref[level_rows(k, o), :]

        u0, v0, t0, t1 = get(UM, 0), get(VM, 0), get(TU, 0), get(TU, 1)
        a1, a2, b1, b2 = roll(u0, 1), roll(u0, 2), roll(u0, -1), roll(u0, -2)
        tl, tr = roll(t0, 1), roll(t0, -1)
        c1, c2, d1, d2 = roll(v0, 1), roll(v0, 2), roll(v0, -1), roll(v0, -2)
        ts = t0 + t1
        tsl = roll(ts, 1)
        um2, um1, up1, up2 = (get(UM, o) for o in (-2, -1, 1, 2))
        vm2, vm1, vp1, vp2 = (get(VM, o) for o in (-2, -1, 1, 2))
        sm, s0, sp = get(TV, -1), get(TV, 0), get(TV, 1)
        cu = mus[k].astype(f32) * FACTOR / (wus[...] * eus[k])
        cv = mvs[k].astype(f32) * FACTOR / (wvs[...] * evs[k])
        du = get(TS, 0) * q(um1, u0, up1, up2) - get(TS, -1) * q(um2, um1, u0, up1)
        dv = (s0 + sp) * q(vm1, v0, vp1, vp2) - (sm + s0) * q(vm2, vm1, v0, vp1)
        du = du + ((t0 + tr) * q(a1, u0, b1, b2) - (tl + t0) * q(a2, a1, u0, b1))
        dv = dv + (ts * q(c1, v0, d1, d2) - tsl * q(c2, c1, v0, d1))
        ou[k] = u0 - cu * du
        ov[k] = v0 - cv * dv
        return cu, cv

    def steps(c, g):
        done = [step(c * LC + 4 * g + i) for i in range(4)]
        cu = jnp.concatenate([d[0] for d in done], axis=0)
        cv = jnp.concatenate([d[1] for d in done], axis=0)
        turned = jnp.where((lanes >= 2) & (lanes <= 5), roll(cv, 4), cu).T
        for row, r in enumerate((C - 2, C - 1, 0, 1, 2, 3, 4, 5)):
            TC[c, row, pl.ds(g, 1), :] = turned[r : r + 1, :]

    def two(h, carry):
        for i in range(2):
            steps(lax.div(h, GB // 2), lax.rem(h, GB // 2) * 2 + i)
        return carry

    lax.fori_loop(0, L // 8, two, 0)

    def edge(x, y, t, s, cu, cv):
        def up(z, o):
            return roll(z, -o)

        f = [(t[a] + t[a + 1]) * q(*x[a : a + 4]) for a in range(3)]
        g = [(t[a] + up(t[a], 1)) * q(*y[a : a + 4]) for a in range(3)]
        out_u, out_v = [], []
        for i in range(2):
            xc, yc = x[i + 2], y[i + 2]
            F = (s[i] + s[i + 1]) * q(up(xc, -1), xc, up(xc, 1), up(xc, 2))
            E = (up(s[i], -1) + s[i]) * q(up(yc, -2), up(yc, -1), yc, up(yc, 1))
            out_u.append(xc - cu[i] * ((f[i + 1] - f[i]) + (F - up(F, -1))))
            out_v.append(yc - cv[i] * ((g[i + 1] - g[i]) + (up(E, 1) - E)))
        return out_u, out_v

    sub = lax.broadcasted_iota(jnp.int32, (8, C), 0)

    def stacked(parts):
        out = jnp.zeros((8, C), f32)
        for r, row in parts:
            out = jnp.where(sub == r, jnp.broadcast_to(row, (8, C)), out)
        return out

    in_edge = (lanes <= 1) | (lanes >= C - 2)

    def unpack(c, g):
        at = pl.ds(g, 1)
        x = [TX[c, i, at, :] for i in range(8)]
        w = [RW[c, f, at, :] for f in range(5)]
        e = [RE[c, f, at, :] for f in range(6)]
        low = stacked(list(enumerate((x[2], x[3], x[4], x[5], x[6], x[7], w[4], e[4]))))
        mid = stacked(list(enumerate((w[0], w[1], e[0], e[1], w[2], w[3], e[2], e[3]))))
        top = stacked(((5, e[5]), (6, x[0]), (7, x[1])))
        turned = jnp.concatenate([low, mid, jnp.zeros((C - 24, C), f32), top], axis=0).T
        first = c * LC + 4 * g
        to = pl.ds(first, 4)
        ou[to] = jnp.where(in_edge, turned, ou[to].reshape(4 * R, C)).reshape(4, R, C)
        ov[to] = jnp.where(in_edge, roll(turned, -4), ov[to].reshape(4 * R, C)).reshape(4, R, C)
        for i in range(4):
            for j, r in enumerate((0, 1, 2, R - 3, R - 2, R - 1)):
                HP[j, pl.ds(first + i, 1), :] = turned[i * R + r : i * R + r + 1, :]

    for c in range(chunks):
        to_east[c].wait_recv()
        to_west[c].wait_recv()
        own = {
            name: (lambda column, table=table: TO[c, table[column]])
            for name, table in (("u", U_COLS), ("v", V_COLS), ("t", T_COLS), ("s", S_COLS))
        }
        eu_, ev_ = edge(
            [own["u"](i) for i in (124, 125, 126, 127)] + [RE[c, 0], RE[c, 1]],
            [own["v"](i) for i in (124, 125, 126, 127)] + [RE[c, 2], RE[c, 3]],
            [own["t"](i) for i in (125, 126, 127)] + [RE[c, 4]],
            [own["s"](i) for i in (126, 127)] + [RE[c, 5]],
            (TC[c, 0], TC[c, 1]), (TC[c, 4], TC[c, 5]),
        )
        wu_, wv_ = edge(
            [RW[c, 0], RW[c, 1]] + [own["u"](i) for i in (0, 1, 2, 3)],
            [RW[c, 2], RW[c, 3]] + [own["v"](i) for i in (0, 1, 2, 3)],
            [RW[c, 4]] + [own["t"](i) for i in (0, 1, 2)],
            [own["s"](i) for i in (0, 1, 2)],
            (TC[c, 2], TC[c, 3]), (TC[c, 6], TC[c, 7]),
        )
        for i, value in enumerate(eu_ + wu_ + ev_ + wv_):
            TX[c, i] = value

        def several(h, carry, c=c):
            for i in range(per):
                unpack(c, h * per + i)
            return carry

        lax.fori_loop(0, GB // per, several, 0)

    @pl.when(has_south)
    def _():
        to_north.wait_recv()
        to_northwest.wait_recv()
        last = stacked(((0, RCS[0:1, :]),))
        KS[...] = jnp.concatenate([last, jnp.zeros((C - 8, C), f32)], axis=0).T[0:L, :]

    @pl.when(jnp.logical_not(has_south))
    def _():
        RS[...] = jnp.zeros_like(RS)
        KS[...] = jnp.zeros_like(KS)

    @pl.when(has_north)
    def _():
        to_south.wait_recv()
        to_southeast.wait_recv()
        first = stacked(((7, RCN[7:8, :]),))
        KN[...] = jnp.concatenate([jnp.zeros((C - 8, C), f32), first], axis=0).T[0:L, :]

    def own_fold(slot):
        G[slot] = SF[...]

    each_fold(lambda slot: fold_copy(slot).wait_recv(), own_fold)

    @pl.when(jnp.logical_not(has_north))
    def _():
        for i in range(6):
            RN[i] = jnp.where(lane < turn, G[0, i], G[1, i])
        KN[...] = G[0, 4]

    col = lax.broadcasted_iota(jnp.int32, (LC, C), 1)

    def left1(x, h):
        return roll(jnp.where(col == C - 1, h, x), 1)

    def left2(x, h):
        return roll(jnp.where(col >= C - 2, h, x), 2)

    def right1(x, h):
        return roll(jnp.where(col == 0, h, x), -1)

    def right2(x, h):
        return roll(jnp.where(col <= 1, h, x), -2)

    def edge_rows(c, carry):
        part = pl.ds(pl.multiple_of(c * LC, 8), LC)

        def own(ref, r):
            return ref[pl.ds(c * LC * pitch + 8 + r, LC, stride=pitch), :]

        def halo(j, shift):
            return roll(HP[j, part, :], shift)

        south = (
            [RS[0, part, :], RS[1, part, :]] + [own(UM, r) for r in range(4)],
            [RS[2, part, :], RS[3, part, :]] + [own(VM, r) for r in range(4)],
            [own(TU, r) for r in range(3)],
            [RS[4, part, :]] + [own(TV, r) for r in range(3)],
            [halo(j, -7) for j in range(3)],
            [KS[part, :], halo(0, 3), halo(1, 3)],
        )
        north = (
            [own(UM, R - 4 + r) for r in range(4)] + [RN[0, part, :], RN[1, part, :]],
            [own(VM, R - 4 + r) for r in range(4)] + [RN[2, part, :], RN[3, part, :]],
            [own(TU, R - 2), own(TU, R - 1), RN[4, part, :]],
            [own(TV, R - 3 + r) for r in range(3)] + [RN[5, part, :]],
            [halo(4, -7), halo(5, -7), KN[part, :]],
            [halo(3, 3), halo(4, 3), halo(5, 3)],
        )
        for side, (x, y, t, s, ht, hs) in enumerate((south, north)):
            F = [(s[a] + right1(s[a], hs[a])) * q(*x[a : a + 4]) for a in range(3)]
            E = [(s[a] + s[a + 1]) * q(*y[a : a + 4]) for a in range(3)]
            for i in range(2):
                p = 2 * side + i
                r = rows[p]
                xc, yc = x[i + 2], y[i + 2]
                hu, hv = halo((0, 1, 4, 5)[p], -10), halo((0, 1, 4, 5)[p], -14)
                a1, a2, b1, b2 = left1(xc, hu), left2(xc, hu), right1(xc, hu), right2(xc, hu)
                c1, c2, d1, d2 = left1(yc, hv), left2(yc, hv), right1(yc, hv), right2(yc, hv)
                du = (t[i] + right1(t[i], ht[i])) * q(a1, xc, b1, b2)
                du = du - (left1(t[i], ht[i]) + t[i]) * q(a2, a1, xc, b1)
                ts, th = t[i] + t[i + 1], ht[i] + ht[i + 1]
                dv = ts * q(c1, yc, d1, d2) - left1(ts, th) * q(c2, c1, yc, d1)
                du = du + (F[i + 1] - F[i])
                dv = dv + (E[i + 1] - E[i])
                cu = pmu[p, part, :].astype(f32) * FACTOR / (wus[r : r + 1, :] * peu[p, part, :])
                cv = pmv[p, part, :].astype(f32) * FACTOR / (wvs[r : r + 1, :] * pev[p, part, :])
                ou[part, r, :] = xc - cu * du
                ov[part, r, :] = yc - cv * dv
        return carry

    lax.fori_loop(0, chunks, edge_rows, 0)

    for c in range(chunks):
        to_east[c].wait_send()
        to_west[c].wait_send()

    @pl.when(has_north)
    def _():
        to_north.wait_send()
        to_northwest.wait_send()

    @pl.when(has_south)
    def _():
        to_south.wait_send()
        to_southeast.wait_send()

    each_fold(lambda slot: fold_copy(slot).wait_send())


def local(n_lat, n_lon, u, v, eu, ev, wu, wv, mu, mv, seam):
    L, R, C = u.shape
    cube = (L, R, C)
    LC = 24 if L % 24 == 0 else 8
    chunks, GB = L // LC, LC // 4
    vm = pltpu.VMEM
    dma = pltpu.SemaphoreType.DMA
    scratch = (
        [vm(cube, f32)] * 4
        + [vm((R, C), f32)] * 2
        + [vm(cube, jnp.int32)] * 2
        + [pltpu.SMEM(seam.shape, jnp.int32)]
        + [vm((4, L, C), f32)] * 2
        + [vm((4, L, C), jnp.int32)] * 2
        + [vm((4, L, C), f32)] * 2
        + [vm((L * (R + 8) + 16, C), f32)] * 5
        + [vm((5, L, C), f32), vm((6, L, C), f32), vm((6, L, C), f32)]
        + [vm((8, C), f32)] * 2
        + [vm((5, L, C), f32), vm((6, L, C), f32)]
        + [vm((8, C), f32)] * 2
        + [vm((2, 6, L, C), f32)]
        + [vm((L, C), f32)] * 2
        + [vm((chunks, OWN, GB, C), f32), vm((chunks, 8, GB, C), f32), vm((chunks, 8, GB, C), f32)]
        + [vm((chunks, 5, GB, C), f32), vm((chunks, 6, GB, C), f32)]
        + [vm((6, L, C), f32)]
        + [dma((chunks, 6)), dma((27,)), dma((4,)), dma((4,)), dma((2,)), dma((2,)), dma((chunks, 2)), dma((chunks, 2))]
    )
    hbm = pl.BlockSpec(memory_space=pltpu.HBM)

    def step(tile, *operands):
        return pl.pallas_call(
            functools.partial(kernel, n_lat, n_lon, L, R, C, LC, tile),
            out_shape=[jax.ShapeDtypeStruct(cube, f32)] * 2,
            in_specs=[hbm] * 9,
            out_specs=[pl.BlockSpec(memory_space=pltpu.VMEM)] * 2,
            scratch_shapes=scratch,
            compiler_params=pltpu.CompilerParams(
                collective_id=tile, has_side_effects=True, vmem_limit_bytes=32 * 1024 * 1024
            ),
        )(*(pltpu.with_memory_space_constraint(x, pltpu.HBM) for x in operands))

    tile = lax.rem((seam[0] + 1) // C, n_lon)
    branches = [functools.partial(step, t) for t in range(n_lon)]
    return tuple(lax.switch(tile, branches, u, v, eu, ev, wu, wv, mu, mv, seam))


def solution(mesh):
    n_lat, n_lon = mesh.shape["lat"], mesh.shape["lon"]
    cube = P(None, "lat", "lon")
    flat = P("lat", "lon")
    return jax.shard_map(
        functools.partial(local, n_lat, n_lon),
        mesh=mesh,
        in_specs=(cube, cube, cube, cube, flat, flat, cube, cube, P()),
        out_specs=(cube, cube),
        check_vma=False,
    )
```

```python
import functools

import jax
import jax.numpy as jnp
from jax import lax
from jax.experimental import pallas as pl
from jax.experimental.pallas import tpu as pltpu
from jax.sharding import PartitionSpec as P

MESH = pl.DeviceIdType.MESH
f32 = jnp.float32

FACTOR = 0.2 * 0.5 / 12.0


EAST = (("U", 126), ("U", 127), ("V", 126), ("V", 127), ("T", 127))
WEST = (("U", 0), ("U", 1), ("V", 0), ("V", 1), ("T", 0), ("S", 0))


def q(a, b, c, d):
    return 7.0 * (b + c) - (a + d)


TP = 144


def roll(x, shift):
    return pltpu.roll(x, shift % x.shape[1], 1)


def kernel(n_lat, n_lon, L, R, C, LC, tile, u, v, eu, ev, wu, wv, mu, mv, seam, ou, ov, *scratch):
    (
        us, vs, eus, evs, wus, wvs, mus, mvs, seams,
        pu, pv, pmu, pmv, peu, pev,
        UM, VM, TU, TV, TS, QA, QB, DV, CU, CV,
        UT, VT, TT, ST, XT, UT2, VT2, FX, GX,
        SN, SS, SF, CN, CS,
        RS, RN, RCS, RCN, G, KS, KN,
        TO, RW, RE,
        in_sem, row_sem, send_sem, recv_sem, fold_send, fold_recv, lon_send, lon_recv,
    ) = scratch
    lat = lax.axis_index("lat")
    lon = lax.axis_index("lon")
    east = lax.rem(lon + 1, n_lon)
    west = lax.rem(lon + n_lon - 1, n_lon)
    has_north = lat < n_lat - 1
    has_south = lat > 0
    pitch = R + 8
    chunks = L // LC
    GB = LC // 4

    rows = (0, 1, R - 2, R - 1)
    loads = [(wu, wus), (wv, wvs), (seam, seams)]
    for src, dst in ((u, pu), (mu, pmu), (v, pv), (mv, pmv), (eu, peu), (ev, pev)):
        for i, r in enumerate(rows):
            loads.append((src.at[:, r, :], dst.at[i]))
    row_copies = [pltpu.make_async_copy(s, d, row_sem.at[i]) for i, (s, d) in enumerate(loads)]
    fields = ((u, us), (mu, mus), (v, vs), (mv, mvs), (eu, eus), (ev, evs))
    full_copies = [
        [
            pltpu.make_async_copy(s.at[pl.ds(c * LC, LC)], d.at[pl.ds(c * LC, LC)], in_sem.at[c, i])
            for i, (s, d) in enumerate(fields)
        ]
        for c in range(chunks)
    ]
    for copy in row_copies:
        copy.start()

    barrier = pltpu.get_barrier_semaphore()

    def greet(a, b):
        pl.semaphore_signal(barrier, inc=1, device_id={"lat": a, "lon": b}, device_id_type=MESH)

    greet(lat, east)
    greet(lat, west)

    @pl.when(has_north)
    def _():
        greet(lat + 1, lon)
        greet(lat + 1, west)

    @pl.when(has_south)
    def _():
        greet(lat - 1, lon)
        greet(lat - 1, east)

    @pl.when(jnp.logical_not(has_north))
    def _():
        for k in range(2, n_lon - 1):
            greet(lat, lax.rem(lon + k, n_lon))

    for copy in row_copies:
        copy.wait()
    for group in full_copies:
        for copy in group:
            copy.start()

    lane = lax.broadcasted_iota(jnp.int32, (L, C), 1)
    um0 = pmu[0].astype(f32) * pu[0]
    um1 = pmu[1].astype(f32) * pu[1]
    vm0 = pmv[0].astype(f32) * pv[0]
    vm1 = pmv[1].astype(f32) * pv[1]
    tu0 = wus[0:1, :] * peu[0] * um0
    SS[0] = um0
    SS[1] = um1
    SS[2] = vm0
    SS[3] = vm1
    SS[4] = tu0
    SS[5] = wvs[0:1, :] * pev[0] * vm0
    um30 = pmu[2].astype(f32) * pu[2]
    um31 = pmu[3].astype(f32) * pu[3]
    vm30 = pmv[2].astype(f32) * pv[2]
    vm31 = pmv[3].astype(f32) * pv[3]
    tv31 = wvs[R - 1 : R, :] * pev[3] * vm31
    SN[0] = um30
    SN[1] = um31
    SN[2] = vm30
    SN[3] = vm31
    SN[4] = tv31
    fill = jnp.zeros((C - L, C), f32)
    CN[...] = jnp.concatenate([tv31, fill], axis=0).T[0:8, :]
    CS[...] = jnp.concatenate([tu0, fill], axis=0).T[C - 8 : C, :]

    turn = lax.rem(seams[0] + 1, C)
    fold_peers = (lax.rem(tile + n_lon - lon, n_lon), lax.rem(tile + 2 * n_lon - 1 - lon, n_lon))

    @pl.when(jnp.logical_not(has_north))
    def _():
        index = (turn + (2 * C - 1) - lane) & (C - 1)
        tu31 = wus[R - 1 : R, :] * peu[3] * um31
        for i, plane in enumerate((um31, um30, vm31, vm30, tu31, tv31)):
            SF[i] = -jnp.take_along_axis(plane, index, axis=1)

    @pl.when(has_north & has_south)
    def _():
        pl.semaphore_wait(barrier, 6)

    @pl.when(jnp.logical_not(has_south))
    def _():
        pl.semaphore_wait(barrier, 4)

    @pl.when(jnp.logical_not(has_north))
    def _():
        pl.semaphore_wait(barrier, n_lon + 1)

    def send(src, dst, i, a, b):
        return pltpu.make_async_remote_copy(
            src_ref=src, dst_ref=dst, send_sem=send_sem.at[i], recv_sem=recv_sem.at[i],
            device_id={"lat": a, "lon": b}, device_id_type=MESH,
        )

    def send_columns(src, dst, c, i, b):
        return pltpu.make_async_remote_copy(
            src_ref=src, dst_ref=dst, send_sem=lon_send.at[c, i], recv_sem=lon_recv.at[c, i],
            device_id={"lat": lat, "lon": b}, device_id_type=MESH,
        )

    to_north = send(SN, RS, 0, lat + 1, lon)
    to_south = send(SS, RN, 1, lat - 1, lon)
    to_northwest = send(CN, RCS, 2, lat + 1, west)
    to_southeast = send(CS, RCN, 3, lat - 1, east)
    to_east = [send_columns(TO.at[c, 0:5], RW.at[c], c, 0, east) for c in range(chunks)]
    to_west = [send_columns(TO.at[c, 5:11], RE.at[c], c, 1, west) for c in range(chunks)]

    def fold_copy(slot):
        return pltpu.make_async_remote_copy(
            src_ref=SF, dst_ref=G.at[slot], send_sem=fold_send.at[slot], recv_sem=fold_recv.at[slot],
            device_id={"lat": lat, "lon": fold_peers[slot]}, device_id_type=MESH,
        )

    def each_fold(act, own=None):
        for slot in range(2):
            mine = fold_peers[slot] == lon

            @pl.when(jnp.logical_not(has_north | mine))
            def _(slot=slot):
                act(slot)

            if own is not None:

                @pl.when(jnp.logical_not(has_north) & mine)
                def _(slot=slot):
                    own(slot)

    each_fold(lambda slot: fold_copy(slot).start())

    @pl.when(has_north)
    def _():
        to_north.start()
        to_northwest.start()

    @pl.when(has_south)
    def _():
        to_south.start()
        to_southeast.start()

    wide_u = jnp.concatenate([wus[...]] * 4, axis=0)
    wide_v = jnp.concatenate([wvs[...]] * 4, axis=0)

    def level_rows(k, o=0):
        return pl.ds(pl.multiple_of(k * pitch + 8, 8) + o, R)

    def columns(b, o, n=C):
        return pl.ds(pl.multiple_of(b * TP + 8, 8) + o, n)

    def pack(c, g):
        first = c * LC + 4 * g
        b = c * GB + g

        def whole(ref):
            return ref[pl.ds(first, 4)].reshape(4 * R, C)

        um = whole(mus).astype(f32) * whole(us)
        vm = whole(mvs).astype(f32) * whole(vs)
        tu = wide_u * whole(eus) * um
        tv = wide_v * whole(evs) * vm
        for i in range(4):
            part = slice(i * R, (i + 1) * R)
            to = level_rows(first + i)
            UM[to, :] = um[part]
            VM[to, :] = vm[part]
            TU[to, :] = tu[part]
            TV[to, :] = tv[part]
        turned = {"U": um.T, "V": vm.T, "T": tu.T, "S": tv.T}
        for name, ref in (("U", UT), ("V", VT), ("T", TT), ("S", ST)):
            ref[columns(b, 0), :] = turned[name]
        for row, (name, column) in enumerate(EAST + WEST):
            TO[c, row, pl.ds(g, 1), :] = turned[name][column : column + 1, :]

    per = 3 if GB % 3 == 0 else 2
    for c in range(chunks):
        for copy in full_copies[c]:
            copy.wait()

        def some(h, carry, c=c):
            for i in range(per):
                pack(c, h * per + i)
            return carry

        lax.fori_loop(0, GB // per, some, 0)
        to_east[c].start()
        to_west[c].start()

    sub = lax.broadcasted_iota(jnp.int32, (8, C), 0)
    lane_c = lax.broadcasted_iota(jnp.int32, (GB, C), 1)
    row_c = lax.broadcasted_iota(jnp.int32, (GB, C), 0)

    def stacked(parts):
        out = jnp.zeros((8, C), f32)
        for r, row in parts:
            out = jnp.where(sub == r, jnp.broadcast_to(row, (8, C)), out)
        return out

    def row_of(r):
        return pl.ds(8 + r, L, stride=pitch)

    def alone(b, carry):
        for i in range(4):
            k = 4 * b + i

            def get(ref, o):
                return ref[level_rows(k, o), :]

            um2, um1, u0, up1, up2 = (get(UM, o) for o in (-2, -1, 0, 1, 2))
            vm2, vm1, v0, vp1, vp2 = (get(VM, o) for o in (-2, -1, 0, 1, 2))
            sm, s0, sp = get(TV, -1), get(TV, 0), get(TV, 1)
            at = level_rows(k)
            QA[at, :] = q(um1, u0, up1, up2)
            QB[at, :] = q(um2, um1, u0, up1)
            DV[at, :] = (s0 + sp) * q(vm1, v0, vp1, vp2) - (sm + s0) * q(vm2, vm1, v0, vp1)
            CU[k] = mus[k].astype(f32) * FACTOR / (wus[...] * eus[k])
            CV[k] = mvs[k].astype(f32) * FACTOR / (wvs[...] * evs[k])
        return carry

    lax.fori_loop(0, L // 4, alone, 0)

    def across(ref, b, o, n=C):
        return ref[columns(b, o, n), :]

    def flux_u(b, o, n):
        return (across(TT, b, o - 1, n) + across(TT, b, o, n)) * q(*(across(UT, b, o + a, n) for a in (-2, -1, 0, 1)))

    def flux_v(b, o, n):
        return across(XT, b, o, n) * q(*(across(VT, b, o + a, n) for a in (-1, 0, 1, 2)))

    def inner_u(b, carry):
        FX[...] = flux_u(b, 0, C + 8)
        UT2[pl.ds(pl.multiple_of(b * C, 8), C), :] = FX[1 : C + 1, :] - FX[0:C, :]
        return carry

    lax.fori_loop(0, L // 4, inner_u, 0)

    @pl.when(has_south)
    def _():
        to_north.wait_recv()
        to_northwest.wait_recv()
        last = stacked(((0, RCS[0:1, :]),))
        KS[...] = jnp.concatenate([last, jnp.zeros((C - 8, C), f32)], axis=0).T[0:L, :]

    @pl.when(jnp.logical_not(has_south))
    def _():
        RS[...] = jnp.zeros_like(RS)
        KS[...] = jnp.zeros_like(KS)

    @pl.when(has_north)
    def _():
        to_south.wait_recv()
        to_southeast.wait_recv()
        KN[...] = RCN[7:8, :]

    def own_fold(slot):
        G[slot] = SF[...]

    each_fold(lambda slot: fold_copy(slot).wait_recv(), own_fold)

    @pl.when(jnp.logical_not(has_north))
    def _():
        for i in range(6):
            RN[i] = jnp.where(lane < turn, G[0, i], G[1, i])
        KN[...] = jnp.concatenate([G[0, 4], fill], axis=0).T[C - 1 : C, :]

    TU[row_of(R), :] = RN[4]
    below = RS[4]
    TS[row_of(-1), :] = below + roll(jnp.where(lane == 0, KS[...], below), -1)

    def edge_rows(c, carry):
        part = pl.ds(pl.multiple_of(c * LC, 8), LC)

        def at(r):
            return pl.ds(c * LC * pitch + 8 + r, LC, stride=pitch)

        def own(ref, first, n):
            return [ref[at(first + r), :] for r in range(n)]

        x = [RS[0, part, :], RS[1, part, :]] + own(UM, 0, 3)
        QB[at(0), :] = q(*x[0:4])
        middle = q(*x[1:5])
        QA[at(0), :] = middle
        QB[at(1), :] = middle
        x = own(UM, R - 3, 3) + [RN[0, part, :], RN[1, part, :]]
        middle = q(*x[0:4])
        QA[at(R - 2), :] = middle
        QB[at(R - 1), :] = middle
        QA[at(R - 1), :] = q(*x[1:5])
        for r, y, t in (
            (0, [RS[2, part, :], RS[3, part, :]] + own(VM, 0, 4), [RS[4, part, :]] + own(TV, 0, 3)),
            (R - 2, own(VM, R - 4, 4) + [RN[2, part, :], RN[3, part, :]], own(TV, R - 3, 3) + [RN[5, part, :]]),
        ):
            E = [(t[a] + t[a + 1]) * q(*y[a : a + 4]) for a in range(3)]
            DV[at(r), :] = E[1] - E[0]
            DV[at(r + 1), :] = E[2] - E[1]
        return carry

    lax.fori_loop(0, chunks, edge_rows, 0)

    def inner_v(h, carry):
        for i in range(per):
            b = h * per + i
            ts = [TU[level_rows(4 * b + j), :] + TU[level_rows(4 * b + j, 1), :] for j in range(4)]
            XT[columns(b, 0), :] = jnp.concatenate(ts, axis=0).T
        for i in range(per):
            b = h * per + i
            GX[...] = flux_v(b, -1, C + 8)
            VT2[pl.ds(pl.multiple_of(b * C, 8), C), :] = GX[1 : C + 1, :] - GX[0:C, :]
        return carry

    lax.fori_loop(0, chunks * GB // per, inner_v, 0)

    spread = lax.broadcasted_iota(jnp.int32, (C, C), 0) % 4 * R + (R - 1)
    spread = jnp.where(spread == lax.broadcasted_iota(jnp.int32, (C, C), 1), 1.0, 0.0).astype(f32)
    for c in range(chunks):
        to_east[c].wait_recv()
        to_west[c].wait_recv()
        corner = jnp.where(lane_c // 4 == row_c + c * GB, jnp.broadcast_to(KN[...], (GB, C)), 0.0)
        corner = lax.dot_general(
            corner, spread, (((1,), (0,)), ((), ())),
            precision=lax.Precision.HIGHEST, preferred_element_type=f32,
        )
        tw = RW[c, 4]
        xw = tw + jnp.where(lane_c % R == R - 1, corner, roll(tw, -1))
        for g in range(GB):
            b = c * GB + g
            row = slice(g, g + 1)
            for ref, o, value in (
                (UT, -2, RW[c, 0, row]), (UT, -1, RW[c, 1, row]),
                (VT, -2, RW[c, 2, row]), (VT, -1, RW[c, 3, row]),
                (TT, -1, RW[c, 4, row]), (XT, -1, xw[row]),
                (UT, C, RE[c, 0, row]), (UT, C + 1, RE[c, 1, row]),
                (VT, C, RE[c, 2, row]), (VT, C + 1, RE[c, 3, row]),
                (TT, C, RE[c, 4, row]), (ST, C, RE[c, 5, row]),
            ):
                ref[b * TP + 8 + o : b * TP + 9 + o, :] = value

    def finish(b):
        def outer(flux, ref, shift):
            at = pl.multiple_of(b * C, 8)
            low = flux(b, shift + 1, 8) - flux(b, shift, 8)
            high = flux(b, C - 7 + shift, 8) - flux(b, C - 8 + shift, 8)
            return jnp.concatenate([low, ref[pl.ds(at + 8, C - 16), :], high], axis=0).T

        du = outer(flux_u, UT2, 0)
        dv = outer(flux_v, VT2, -1)
        ts = (across(ST, b, 0) + across(ST, b, 1)).T
        for i in range(4):
            k = 4 * b + i
            part = slice(i * R, (i + 1) * R)
            at = level_rows(k)
            TS[at, :] = ts[part]
            step = du[part] + ts[part] * QA[at, :] - TS[level_rows(k, -1), :] * QB[at, :]
            ou[k] = UM[at, :] - CU[k] * step
            ov[k] = VM[at, :] - CV[k] * (dv[part] + DV[at, :])

    def some_blocks(h, carry):
        for i in range(per):
            finish(h * per + i)
        return carry

    lax.fori_loop(0, chunks * GB // per, some_blocks, 0)

    for c in range(chunks):
        to_east[c].wait_send()
        to_west[c].wait_send()

    @pl.when(has_north)
    def _():
        to_north.wait_send()
        to_northwest.wait_send()

    @pl.when(has_south)
    def _():
        to_south.wait_send()
        to_southeast.wait_send()

    each_fold(lambda slot: fold_copy(slot).wait_send())


PIECES = 4


def write_out(L, nu, nv, ou, ov, sem):
    n = L // PIECES
    copies = [
        pltpu.make_async_copy(src.at[pl.ds(p * n, n)], dst.at[pl.ds(p * n, n)], sem.at[i, p])
        for p in range(PIECES)
        for i, (src, dst) in enumerate(((nu, ou), (nv, ov)))
    ]
    for copy in copies:
        copy.start()
    for copy in copies:
        copy.wait()


def local(n_lat, n_lon, u, v, eu, ev, wu, wv, mu, mv, seam):
    L, R, C = u.shape
    cube = (L, R, C)
    LC = 24 if L % 24 == 0 else 8
    chunks, GB = L // LC, LC // 4
    vm = pltpu.VMEM
    dma = pltpu.SemaphoreType.DMA
    scratch = (
        [vm(cube, f32)] * 4
        + [vm((R, C), f32)] * 2
        + [vm(cube, jnp.int32)] * 2
        + [pltpu.SMEM(seam.shape, jnp.int32)]
        + [vm((4, L, C), f32)] * 2
        + [vm((4, L, C), jnp.int32)] * 2
        + [vm((4, L, C), f32)] * 2
        + [vm((L * (R + 8) + 16, C), f32)] * 8
        + [vm(cube, f32)] * 2
        + [vm((chunks * GB * TP + 8, C), f32)] * 5
        + [vm((chunks * GB * C, C), f32)] * 2
        + [vm((C + 8, C), f32)] * 2
        + [vm((5, L, C), f32), vm((6, L, C), f32), vm((6, L, C), f32)]
        + [vm((8, C), f32)] * 2
        + [vm((5, L, C), f32), vm((6, L, C), f32)]
        + [vm((8, C), f32)] * 2
        + [vm((2, 6, L, C), f32)]
        + [vm((L, C), f32), vm((1, C), f32)]
        + [vm((chunks, 11, GB, C), f32)]
        + [vm((chunks, 5, GB, C), f32), vm((chunks, 6, GB, C), f32)]
        + [dma((chunks, 6)), dma((27,)), dma((4,)), dma((4,)), dma((2,)), dma((2,)), dma((chunks, 2)), dma((chunks, 2))]
    )
    hbm = pl.BlockSpec(memory_space=pltpu.HBM)

    def step(tile, *operands):
        return pl.pallas_call(
            functools.partial(kernel, n_lat, n_lon, L, R, C, LC, tile),
            out_shape=[jax.ShapeDtypeStruct(cube, f32)] * 2,
            in_specs=[hbm] * 9,
            out_specs=[pl.BlockSpec(memory_space=pltpu.VMEM)] * 2,
            scratch_shapes=scratch,
            compiler_params=pltpu.CompilerParams(
                collective_id=tile, has_side_effects=True, vmem_limit_bytes=44 * 1024 * 1024
            ),
        )(*(pltpu.with_memory_space_constraint(x, pltpu.HBM) for x in operands))

    tile = lax.rem((seam[0] + 1) // C, n_lon)
    branches = [functools.partial(step, t) for t in range(n_lon)]
    nu, nv = lax.switch(tile, branches, u, v, eu, ev, wu, wv, mu, mv, seam)
    return tuple(
        pl.pallas_call(
            functools.partial(write_out, L),
            out_shape=[jax.ShapeDtypeStruct(cube, f32)] * 2,
            in_specs=[pl.BlockSpec(memory_space=pltpu.VMEM)] * 2,
            out_specs=[hbm] * 2,
            scratch_shapes=[dma((2, PIECES))],
            compiler_params=pltpu.CompilerParams(vmem_limit_bytes=1024 * 1024),
        )(*(pltpu.with_memory_space_constraint(x, pltpu.VMEM) for x in (nu, nv)))
    )


def solution(mesh):
    n_lat, n_lon = mesh.shape["lat"], mesh.shape["lon"]
    cube = P(None, "lat", "lon")
    flat = P("lat", "lon")
    return jax.shard_map(
        functools.partial(local, n_lat, n_lon),
        mesh=mesh,
        in_specs=(cube, cube, cube, cube, flat, flat, cube, cube, P()),
        out_specs=(cube, cube),
        check_vma=False,
    )
```
